32 devices in a mesh: space: 16 (over z, y, x), rep: 2 (over core).
Axes of the slice: x: 2, y: 2, z: 4, core: 2. Of those that a mesh axis runs over, the one named last changes fastest.
Arguments:
- halo_rows: bfloat16 [4, 2048, 256], P(None, 'space', 'rep'), may hold values from -6 to 6
- unmatched: int32 [4, 2048], P(None, 'space'), may hold values 0 or 1
- owner_id: int32 [4, 2048, 1], P(None, 'space'), may hold values from 0 to 15; in each aligned block of 128 rows (0 to 127, 128 to 255, ..., all dimensions but the last counted through in order) at most 16 rows name the same one
- cand_index: int32 [4, 2048, 16], P(None, 'space'), may hold values from 0 to 511
- lengths: int32 [4, 2048], P(None, 'space'), may hold values from 1 to 16
- choice_index: int32 [4, 2048], P(None, 'space'), may hold values from 0 to 15, as said below
- desc_rows: bfloat16 [4, 8192, 256], P(None, 'space', 'rep'), may hold values from -6 to 6
Outputs:
- phantom: bfloat16 [4, 2048, 256], P(None, 'space', 'rep')
- best_merit: bfloat16 [4, 2048], P(None, 'space')
The draws below stay inside these ranges and needn't reach their ends.
Inputs may be any that keep to these rules, and one draw needn't show every extreme that they name: `owner_id`: in each aligned block of 128 halos (one region in one snapshot) no owner is named by more than 16 halos, a bound that some block reaches. `choice_index`: less than the halo's length.
All inputs are finite; a program needn't handle non-finite values. No bound on the sum of `unmatched` on one device may be relied on, other than what follows from the above.
Results may differ from the reference program's by a relative error of at most 0.001.
Values may be sent and summed in bfloat16 or wider, within the bound.
A program may use at most 64 MiB of HBM per device.

```python
import math
import jax
import jax.numpy as jnp
import numpy as np
from jax import lax

WIDTH = 256
SNAPS = 4
K = 16
HALO_DEV = 128
CAND_DEV = 512
CAP = 16
HALOS = 2048
CANDS = 8192
N_SPACE = 16


def draw_pair(key):
    base_key = jax.random.fold_in(key, 71)
    first_key, second_key = jax.random.split(base_key)
    span_draw = jax.random.randint(first_key, (SNAPS, HALOS), 1, K + 1)
    pick_draw = jax.random.randint(second_key, (SNAPS, HALOS), 0, 1048576) % span_draw
    return (span_draw, pick_draw)


def draw_lengths(key, part):
    return draw_pair(key)[0].astype(jnp.int32)


def draw_choice_index(key, part):
    return draw_pair(key)[1].astype(jnp.int32)


def place_ends(values, rng, smallest, top_value):
    shape = values.shape
    index_at = [jax.random.randint(jax.random.fold_in(rng, axis), (), 0, shape[axis]) for axis in range(len(shape))]
    values = values.at[tuple(index_at)].set(smallest)
    longest = shape.index(max(shape))
    index_at[longest] = (index_at[longest] + 1) % shape[longest]
    return values.at[tuple(index_at)].set(top_value)


def shard_levels(stream_key, extent, shards, low, largest):
    level, own = 1.0, jax.random.fold_in(stream_key, 6)
    for position, parts in shards:
        draws = jnp.exp(jax.random.uniform(jax.random.fold_in(own, position), (parts,), jnp.float32, low / len(shards), largest / len(shards)))
        level = level * jnp.repeat(draws, extent[position] // parts).reshape([-1 if axis == position else 1 for axis in range(len(extent))])
    return level


def routed_block(own_key, own, number, rows, count, top, limit, skew):
    order = jax.random.permutation(own_key, count)
    packed, common = shares(count, rows * top, limit, skew, True), shares(count, rows * top, limit, skew, False)
    places = jnp.arange(count)

    def named(tallies, offset_by):
        used = int((tallies > 0).sum())
        fixed = max(1, used // 4)
        passed = fixed + (places - fixed + offset_by * (used - fixed)) % max(1, count - fixed)
        return jnp.zeros((count,), jnp.int32).at[order[jnp.where(places < fixed, places, passed)]].set(jnp.asarray(tallies, jnp.int32))

    tallies = jnp.where(number % 4 == 0, named(packed, number // 4), named(common, number - number // 4 - 1))
    mixed = jax.random.permutation(jax.random.fold_in(own, 3), count)
    giver, receiver = mixed[0:count // 2 * 2:2], mixed[1:count // 2 * 2:2]
    room = jnp.minimum(tallies[giver] - 1, limit - tallies[receiver]) // 2
    room = jnp.where((giver == order[0]) | (receiver == order[0]) | (tallies[receiver] == 0), 0, jnp.maximum(room, 0))
    passed = jax.random.randint(jax.random.fold_in(own, 4), (count // 2,), 0, 1 << 20) % (room + 1)
    tallies = tallies.at[giver].add(-passed).at[receiver].add(passed)
    items = jnp.searchsorted(jnp.cumsum(tallies), jnp.arange(rows * top), side="right").astype(jnp.int32)
    grid = items.reshape(top, rows).T
    grid = grid[jax.random.permutation(jax.random.fold_in(own, 1), rows)]
    offset_by = jax.random.randint(jax.random.fold_in(own, 2), (rows, 1), 0, top)
    return jnp.take_along_axis(grid, (jnp.arange(top)[None, :] + offset_by) % top, axis=1)


def shares(amount, total, limit, slope, full):
    portions = [(1 << 20) // math.isqrt(rank ** slope) + 1 for rank in range(1, amount + 1)]
    largest = limit if full else min(limit, max(-(-total // amount), total * portions[0] // sum(portions)))
    least = 1 if total - largest >= amount - 1 else 0
    counts, rest = [largest] + [least] * (amount - 1), total - largest - least * (amount - 1)
    while rest > 0:
        movable = [i for i in range(1, amount) if counts[i] < largest] or [i for i in range(1, amount) if counts[i] < limit]
        pool, budget = sum([portions[i] for i in movable]), rest
        for i in movable:
            extra = min(limit - counts[i], max(1, budget * portions[i] // pool), rest)
            counts[i] = counts[i] + extra
            rest = rest - extra
    return np.array(counts)


def noise(own_key, dims, deviation, bound, shards=(), kind=jnp.bfloat16):
    entries = jax.random.normal(own_key, dims, jnp.float32) * deviation
    if len(shards) > 0:
        entries = shard_levels(own_key, dims, shards, -0.22, 0.18) * entries
    return jnp.clip(entries, min=-bound, max=bound).astype(kind)


def setup_inputs(seed: int = 0) -> dict:
    splits = jax.random.split(jax.random.key(seed), 8)
    halo_rows = noise(splits[0], (SNAPS, HALOS, WIDTH), 1.0, 6.0, ((1, 16), (2, 2)))
    unmatched = place_ends((jax.random.randint(splits[1], (SNAPS, HALOS), 0, 3) < 2).astype(jnp.int32), jax.random.fold_in(splits[1], 1), 0, 1)
    owner_id_keys = jax.random.split(jax.random.fold_in(splits[2], 1), SNAPS * HALOS // HALO_DEV)
    owner_id_turns = jax.random.permutation(jax.random.fold_in(splits[2], 3), SNAPS * HALOS // HALO_DEV)
    owner_id = jax.vmap(lambda own, number: routed_block(jax.random.fold_in(splits[2], 2), own, number, HALO_DEV, N_SPACE, 1, CAP, 2))(owner_id_keys, owner_id_turns).reshape((SNAPS, HALOS, 1))
    cand_index = place_ends(jax.random.randint(splits[3], (SNAPS, HALOS, K), 0, CAND_DEV), jax.random.fold_in(splits[3], 1), 0, CAND_DEV - 1).astype(jnp.int32)
    lengths = draw_lengths(jax.random.fold_in(splits[7], 71), 0)
    choice_index = draw_choice_index(jax.random.fold_in(splits[7], 71), 0)
    desc_rows = noise(splits[6], (SNAPS, CANDS, WIDTH), 1.0, 6.0, ((1, 16), (2, 2)))
    return dict(halo_rows=halo_rows, unmatched=unmatched, owner_id=owner_id, cand_index=cand_index, lengths=lengths, choice_index=choice_index, desc_rows=desc_rows)


def reference(halo_rows, unmatched, owner_id, cand_index, lengths, choice_index, desc_rows):
    phantom_list = []
    best_list = []
    lane_ids = jnp.arange(K, dtype=jnp.int32)
    block_size = math.gcd(HALOS, 4096)
    for snapshot in range(SNAPS):
        rows_here = halo_rows[snapshot]
        desc_table = desc_rows[snapshot]
        glob = (owner_id[snapshot, :, 0][:, None] * CAND_DEV + cand_index[snapshot]).astype(jnp.int32)

        def score_block(pieces):
            rows_block, glob_block = pieces
            picked = desc_table[glob_block].astype(jnp.float32)
            return jnp.einsum('rkw,rw->rk', picked, rows_block.astype(jnp.float32))
        merit_full = lax.map(score_block, (rows_here.reshape(-1, block_size, WIDTH), glob.reshape(-1, block_size, K)))
        merit_full = merit_full.reshape(HALOS, K) / math.sqrt(WIDTH)
        live_halo = unmatched[snapshot] == 1
        used = lane_ids[None, :] < lengths[snapshot][:, None]
        live_entry = used & live_halo[:, None]
        quality = 1.0 + jax.nn.softplus(merit_full)
        claims = jnp.zeros((CANDS,), jnp.float32).at[glob.reshape(-1)].max(jnp.where(live_entry, quality, jnp.zeros_like(quality)).reshape(-1))
        pick_pos = choice_index[snapshot][:, None].astype(jnp.int32)
        chosen = jnp.take_along_axis(glob, pick_pos, 1)[:, 0]
        chosen_quality = jnp.take_along_axis(quality, pick_pos, 1)[:, 0]
        share_weight = chosen_quality / (chosen_quality + claims[chosen])
        blended = ((1.0 - share_weight)[:, None] * rows_here.astype(jnp.float32) + share_weight[:, None] * desc_table[chosen].astype(jnp.float32)).astype(jnp.bfloat16)
        phantom_list.append(jnp.where(live_halo[:, None], blended, rows_here))
        top_merit = lax.optimization_barrier(jnp.max(jnp.where(used, merit_full, jnp.full_like(merit_full, -1e+30)), axis=1))
        best_list.append(jnp.where(live_halo, top_merit, jnp.zeros_like(top_merit)).astype(jnp.bfloat16))
    return (jnp.stack(phantom_list), jnp.stack(best_list))
```

```python
import functools
import math

import jax
import jax.numpy as jnp
from jax import lax
from jax.experimental import pallas as pl
from jax.experimental.pallas import tpu as pltpu
from jax.sharding import PartitionSpec as P

MESH = pl.DeviceIdType.MESH
F32 = jnp.float32
BF16 = jnp.bfloat16
NEG = -1e30
GROUP = 32
NT = (((1,), (1,)), ((), ()))
TN = (((0,), (0,)), ((), ()))


def iota(shape, dim):
    return lax.broadcasted_iota(jnp.int32, shape, dim)


def dot(a, b):
    return jnp.dot(a, b, preferred_element_type=F32)


def hot(mask):
    return jnp.where(mask, 1.0, 0.0).astype(BF16)


def code(index, cands):
    return index - cands // 2 + jnp.where(index >= cands // 2, 1, 0)


def kernel(
    n, slots, width,
    halo, unmatched, owner, cand, lengths, choice, desc,
    phantom, best,
    send, recv, send_meta, recv_meta, table, scores, back, recv_back, back_best, recv_best,
    row_ss, row_rs, meta_ss, meta_rs, back_ss, back_rs, best_ss, best_rs, table_sem, local_sem,
):
    me, core = lax.axis_index("space"), lax.axis_index("rep")
    snaps, halos, half = halo.shape
    k_count = cand.shape[1]
    cands = desc.shape[1]
    own = snaps // 2
    total = n * slots

    def core_of(x):
        return lax.rem(core + x, 2)

    def remote(src, dst, ss, rs, peer, x):
        return pltpu.make_async_remote_copy(
            src_ref=src, dst_ref=dst, send_sem=ss, recv_sem=rs,
            device_id=(peer, core_of(x)), device_id_type=MESH,
        )

    def each_peer(f):
        @pl.loop(1, n)
        def _(d):
            peer = lax.rem(me + d, n)
            f(peer, 0)
            f(peer, 1)

        f(me, 1)

    def each_chip(f):
        @pl.loop(1, n)
        def _(d):
            f(lax.rem(me + d, n))

    barrier = pltpu.get_barrier_semaphore()
    each_peer(
        lambda peer, x: pl.semaphore_signal(
            barrier, inc=1, device_id=(peer, core_of(x)), device_id_type=MESH
        )
    )

    upper = hot(iota((halos, halos), 0) < iota((halos, halos), 1))
    route = []
    for x in range(2):
        for ls in range(own):
            s = own * core_of(x) + ls
            dest = owner[s]
            named = iota((n, halos), 0) == dest
            onehot = hot(named)
            rank = jnp.sum(jnp.where(named, dot(onehot, upper), 0.0), axis=0, keepdims=True)
            rank = rank.astype(jnp.int32)
            live = unmatched[pl.ds(s, 1), :] == 1
            target = jnp.where(live, dest * slots + rank, -1)
            route.append((onehot, rank, target, live))

    meta = None
    for x in range(2):
        for ls in range(own):
            s = own * core_of(x) + ls
            _, _, target, live = route[x * own + ls]
            place = hot(iota((total, halos), 0) == target)
            rows = dot(place, halo[s]).astype(BF16)
            send[x, :, ls * slots : (ls + 1) * slots, :] = rows.reshape(n, slots, half)
            if x == 0:
                listed = code(cand[s], cands)
                k_ids = iota((k_count, halos), 0)
                pick = jnp.sum(
                    jnp.where(k_ids == choice[pl.ds(s, 1), :], listed, 0), axis=0, keepdims=True
                )
                listed = jnp.where(k_ids < lengths[pl.ds(s, 1), :], listed, 0)
                block = jnp.concatenate(
                    [listed, jnp.broadcast_to(pick, (GROUP - k_count, halos))], axis=0
                ).astype(F32)
                parts = [block]
                if ls > 0:
                    parts.insert(0, jnp.zeros((ls * GROUP, halos), F32))
                parts.append(jnp.zeros((128 - (ls + 1) * GROUP, halos), F32))
                block = jnp.concatenate(parts, axis=0).astype(BF16)
                term = lax.dot_general(place, block, NT, preferred_element_type=F32)
                meta = term if meta is None else meta + term
    send_meta[...] = meta.astype(BF16).reshape(n, slots, 128)

    pl.semaphore_wait(barrier, 2 * n - 1)

    def row_copy(peer, x):
        return remote(send.at[x, peer], recv.at[x, me], row_ss.at[x, peer], row_rs.at[x, me], peer, x)

    def row_arrival(peer, x):
        return remote(send.at[x, peer], recv.at[x, peer], row_ss.at[x, peer], row_rs.at[x, peer], peer, x)

    def meta_copy(peer):
        return remote(send_meta.at[peer], recv_meta.at[me], meta_ss.at[peer], meta_rs.at[me], peer, 0)

    def meta_arrival(peer):
        return remote(send_meta.at[peer], recv_meta.at[peer], meta_ss.at[peer], meta_rs.at[peer], peer, 0)

    each_chip(lambda peer: meta_copy(peer).start())
    each_peer(lambda peer, x: row_copy(peer, x).start())
    table_copy = remote(
        desc.at[pl.ds(own * core_of(1), own)], table, table_sem.at[0], table_sem.at[1], me, 1
    )
    table_copy.start()
    local_row = pltpu.make_async_copy(send.at[0, me], recv.at[0, me], local_sem.at[0])
    local_meta = pltpu.make_async_copy(send_meta.at[me], recv_meta.at[me], local_sem.at[1])
    local_row.start()
    local_meta.start()

    local_row.wait()
    local_meta.wait()
    table_copy.wait_recv()
    each_chip(lambda peer: meta_arrival(peer).wait_recv())
    each_peer(lambda peer, x: row_arrival(peer, x).wait_recv())

    meta_all = recv_meta[...].reshape(total, 128).astype(F32)
    meta_rows = meta_all.T
    step = 64
    fold = None
    for ls in range(own):
        s = own * core + ls
        halves = [
            recv[x, :, ls * slots : (ls + 1) * slots, :].reshape(total, half) for x in range(2)
        ]
        tables = [desc[s], table[ls]]
        scores[...] = lax.dot_general(
            jnp.concatenate(tables, axis=1), jnp.concatenate(halves, axis=1), NT,
            preferred_element_type=F32,
        )
        lists = meta_rows[ls * GROUP : ls * GROUP + k_count]
        pick = meta_rows[ls * GROUP + k_count : ls * GROUP + k_count + 1]

        def chunk(i, carry):
            top, picked, claimed = carry
            ids = code(iota((step, total), 0) + i * step, cands).astype(F32)
            value = scores[pl.ds(pl.multiple_of(i * step, step), step), :]
            mask = ids == lists[0:1]
            for k in range(1, k_count):
                mask = mask | (ids == lists[k : k + 1])
            masked = jnp.where(mask, value, NEG)
            claim = jnp.max(masked, axis=1, keepdims=True)
            chosen = ids == pick

            def least(v):
                return jnp.max(v.reshape(step // 8, 8, total), axis=0)

            return (
                jnp.maximum(top, least(masked)),
                jnp.maximum(picked, least(jnp.where(chosen, value, NEG))),
                jnp.maximum(claimed, least(jnp.where(chosen, claim, NEG))),
            )

        start = jnp.full((8, total), NEG, F32)
        top, picked, claimed = [
            jnp.max(v, axis=0, keepdims=True)
            for v in lax.fori_loop(0, cands // step, chunk, (start, start, start))
        ]

        def quality(v):
            v = v * (1.0 / math.sqrt(width))
            return 1.0 + jnp.maximum(v, 0.0) + jnp.log(1.0 + jnp.exp(-jnp.abs(v)))

        mine = quality(picked)
        share = mine / (mine + quality(claimed))
        share = jnp.broadcast_to(share, (128, total)).T
        column = meta_all[:, ls * GROUP + k_count : ls * GROUP + k_count + 1]
        select = hot(column == code(iota((total, cands), 1), cands).astype(F32))
        for x in range(2):
            taken = dot(select, tables[x])
            blend = (1.0 - share) * halves[x].astype(F32) + share * taken
            back[x, :, ls * slots : (ls + 1) * slots, :] = blend.astype(BF16).reshape(n, slots, half)

        top = jnp.where(top > NEG * 0.5, top * (1.0 / math.sqrt(width)), 0.0)
        spread = jnp.where(
            iota((n, total), 0) == iota((n, total), 1) // slots, jnp.broadcast_to(top, (n, total)), 0.0
        ).astype(BF16)
        lane = iota((total, 128), 0)
        term = dot(spread, hot(iota((total, 128), 1) == ls * slots + lane % slots))
        fold = term if fold is None else fold + term
    back_best[...] = fold.reshape(n, 1, 128)

    def back_copy(peer, x):
        return remote(back.at[x, peer], recv_back.at[x, me], back_ss.at[x, peer], back_rs.at[x, me], peer, x)

    def back_arrival(peer, x):
        return remote(back.at[x, peer], recv_back.at[x, peer], back_ss.at[x, peer], back_rs.at[x, peer], peer, x)

    def best_copy(peer, x):
        return remote(back_best.at[peer], recv_best.at[x, me], best_ss.at[x, peer], best_rs.at[x, me], peer, x)

    def best_arrival(peer, x):
        return remote(back_best.at[peer], recv_best.at[x, peer], best_ss.at[x, peer], best_rs.at[x, peer], peer, x)

    each_peer(lambda peer, x: back_copy(peer, x).start())
    each_peer(lambda peer, x: best_copy(peer, x).start())
    local_back = pltpu.make_async_copy(back.at[0, me], recv_back.at[0, me], local_sem.at[2])
    local_best = pltpu.make_async_copy(back_best.at[me], recv_best.at[0, me], local_sem.at[3])
    local_back.start()
    local_best.start()
    local_back.wait()
    local_best.wait()
    each_peer(lambda peer, x: back_arrival(peer, x).wait_recv())
    each_peer(lambda peer, x: best_arrival(peer, x).wait_recv())

    tops = []
    for x in range(2):
        brought = recv_best[x].reshape(n, 128).astype(BF16)
        for ls in range(own):
            s = own * core_of(x) + ls
            onehot, rank, target, live = route[x * own + ls]
            column = jnp.broadcast_to(target.astype(F32), (128, halos)).T[:, 0:1]
            place = hot(iota((halos, total), 1).astype(F32) == column)
            rows = dot(place, recv_back[x, :, ls * slots : (ls + 1) * slots, :].reshape(total, half))
            phantom[s] = jnp.where(column < 0.0, halo[s].astype(F32), rows).astype(BF16)
            spread = lax.dot_general(brought, onehot, TN, preferred_element_type=F32)
            here = jnp.where(iota((128, halos), 0) == ls * slots + rank, spread, 0.0)
            tops.append(jnp.where(live, jnp.sum(here, axis=0, keepdims=True), 0.0))
    first, second = jnp.concatenate(tops[:own], axis=0), jnp.concatenate(tops[own:], axis=0)
    even = core == 0
    best[...] = jnp.concatenate(
        [jnp.where(even, first, second), jnp.where(even, second, first)], axis=0
    ).astype(BF16)

    table_copy.wait_send()
    each_chip(lambda peer: meta_copy(peer).wait_send())
    each_peer(lambda peer, x: row_copy(peer, x).wait_send())
    each_peer(lambda peer, x: back_copy(peer, x).wait_send())
    each_peer(lambda peer, x: best_copy(peer, x).wait_send())


def body(n, halo_rows, unmatched, owner_id, cand_index, lengths, choice_index, desc_rows):
    snaps, halos, half = halo_rows.shape
    cands = desc_rows.shape[1]
    own = snaps // 2
    slots = max(2 * halos // n, 16)
    total = n * slots
    dma = pltpu.SemaphoreType.DMA
    return pl.pallas_call(
        functools.partial(kernel, n, slots, 2 * half),
        out_shape=(
            jax.ShapeDtypeStruct((snaps, halos, half), BF16),
            jax.ShapeDtypeStruct((snaps, halos), BF16),
        ),
        in_specs=[pl.BlockSpec(memory_space=pltpu.VMEM)] * 7,
        out_specs=(pl.BlockSpec(memory_space=pltpu.VMEM),) * 2,
        scratch_shapes=[
            pltpu.VMEM((2, n, own * slots, half), BF16),
            pltpu.VMEM((2, n, own * slots, half), BF16),
            pltpu.VMEM((n, slots, 128), BF16),
            pltpu.VMEM((n, slots, 128), BF16),
            pltpu.VMEM((own, cands, half), BF16),
            pltpu.VMEM((cands, total), F32),
            pltpu.VMEM((2, n, own * slots, half), BF16),
            pltpu.VMEM((2, n, own * slots, half), BF16),
            pltpu.VMEM((n, 1, 128), F32),
            pltpu.VMEM((2, n, 1, 128), F32),
            dma((2, n)), dma((2, n)), dma((n,)), dma((n,)),
            dma((2, n)), dma((2, n)), dma((2, n)), dma((2, n)),
            dma((2,)), dma((4,)),
        ],
        compiler_params=pltpu.CompilerParams(collective_id=0, has_side_effects=True),
    )(
        halo_rows,
        unmatched,
        jnp.swapaxes(owner_id, 1, 2),
        jnp.swapaxes(cand_index, 1, 2),
        lengths,
        choice_index,
        desc_rows,
    )


def solution(mesh):
    in_specs = (
        P(None, "space", "rep"),
        P(None, "space"),
        P(None, "space", None),
        P(None, "space", None),
        P(None, "space"),
        P(None, "space"),
        P(None, "space", "rep"),
    )
    out_specs = (P(None, "space", "rep"), P(None, "space"))
    return jax.shard_map(
        functools.partial(body, mesh.shape["space"]),
        mesh=mesh, in_specs=in_specs, out_specs=out_specs, check_vma=False,
    )
```

```python
import functools
import math

import jax
import jax.numpy as jnp
from jax import lax
from jax.experimental import pallas as pl
from jax.experimental.pallas import tpu as pltpu
from jax.sharding import PartitionSpec as P

MESH = pl.DeviceIdType.MESH
F32 = jnp.float32
BF16 = jnp.bfloat16
NEG = -1e30
GROUP = 32
NT = (((1,), (1,)), ((), ()))
TN = (((0,), (0,)), ((), ()))


def iota(shape, dim):
    return lax.broadcasted_iota(jnp.int32, shape, dim)


def dot(a, b):
    return jnp.dot(a, b, preferred_element_type=F32)


def hot(mask):
    return jnp.where(mask, 1.0, 0.0).astype(BF16)


def code(index, cands):
    return index - cands // 2 + jnp.where(index >= cands // 2, 1, 0)


def kernel(
    n, slots, width,
    halo, unmatched, owner, cand, lengths, choice, desc,
    phantom, best,
    send, recv, send_meta, recv_meta, mine_table, table, scores, bias, taken,
    back, recv_back, back_best, recv_best,
    row_ss, row_rs, meta_ss, meta_rs, back_ss, back_rs, best_ss, best_rs, table_sem, local_sem,
):
    me, core = lax.axis_index("space"), lax.axis_index("rep")
    snaps, halos, half = halo.shape
    k_count = cand.shape[1]
    cands = desc.shape[1]
    own = snaps // 2
    total = n * slots
    hs = slots // 2

    def core_of(x):
        return lax.rem(core + x, 2)

    def remote(src, dst, ss, rs, peer, x):
        return pltpu.make_async_remote_copy(
            src_ref=src, dst_ref=dst, send_sem=ss, recv_sem=rs,
            device_id=(peer, core_of(x)), device_id_type=MESH,
        )

    bits = n.bit_length() - 1
    mine_bits = [lax.rem(lax.div(me, 1 << i), 2) for i in range(bits)]

    def far_first(f):
        @pl.loop(1, n)
        def _(d):
            if n == 1 << bits:
                m = n - d
                peer = 0
                for i in range(bits):
                    flip = lax.rem(lax.div(m, 1 << i), 2)
                    peer = peer + (mine_bits[i] + flip - 2 * mine_bits[i] * flip) * (1 << i)
            else:
                peer = lax.rem(me + d, n)
            f(peer)

    def each_chip(f):
        @pl.loop(1, n)
        def _(d):
            f(lax.rem(me + d, n))

    def each_peer(f, order=each_chip):
        def both(peer):
            f(peer, 0)
            f(peer, 1)

        order(both)
        f(me, 1)

    barrier = pltpu.get_barrier_semaphore()
    each_peer(
        lambda peer, x: pl.semaphore_signal(
            barrier, inc=1, device_id=(peer, core_of(x)), device_id_type=MESH
        ),
        far_first,
    )
    own_table = pltpu.make_async_copy(desc.at[pl.ds(own * core, own)], mine_table, local_sem.at[0])
    own_table.start()

    upper = hot(iota((halos, halos), 0) < iota((halos, halos), 1))
    route = []
    for x in range(2):
        for ls in range(own):
            s = own * core_of(x) + ls
            dest = owner[s]
            named = iota((n, halos), 0) == dest
            onehot = hot(named)
            rank = jnp.sum(jnp.where(named, dot(onehot, upper), 0.0), axis=0, keepdims=True)
            rank = rank.astype(jnp.int32)
            live = unmatched[pl.ds(s, 1), :] == 1
            target = jnp.where(live, dest * slots + rank, -1)
            route.append((onehot, rank, target, live))

    meta = None
    for ls in range(own):
        s = own * core + ls
        _, rank, _, live = route[ls]
        listed = code(cand[s], cands)
        k_ids = iota((k_count, halos), 0)
        pick = jnp.sum(jnp.where(k_ids == choice[pl.ds(s, 1), :], listed, 0), axis=0, keepdims=True)
        listed = jnp.where(k_ids < lengths[pl.ds(s, 1), :], listed, 0)
        block = jnp.concatenate(
            [listed, jnp.broadcast_to(pick, (GROUP - k_count, halos))], axis=0
        ).astype(F32)
        for g in range(2):
            lead = (g * own + ls) * GROUP
            parts = [jnp.zeros((lead, halos), F32)] if lead else []
            parts.append(block)
            if lead + GROUP < 128:
                parts.append(jnp.zeros((128 - lead - GROUP, halos), F32))
            here = live & (rank >= g * hs) & (rank < (g + 1) * hs)
            row = jnp.where(here, owner[s] * hs + rank - g * hs, -1)
            term = lax.dot_general(
                hot(iota((n * hs, halos), 0) == row),
                (jnp.concatenate(parts, axis=0) if len(parts) > 1 else block).astype(BF16),
                NT, preferred_element_type=F32,
            )
            meta = term if meta is None else meta + term
    send_meta[...] = meta.astype(BF16).reshape(n, hs, 128)

    for ls in range(own):
        for x in range(2):
            place = hot(iota((total, halos), 0) == route[x * own + ls][2])
            rows = dot(place, halo[own * core_of(x) + ls]).astype(BF16)
            send[ls, x] = rows.reshape(n, slots, half)

    pl.semaphore_wait(barrier, 2 * n - 1)

    def row_copy(ls, peer, x, at):
        return remote(
            send.at[ls, x, peer], recv.at[ls, x, at], row_ss.at[ls, x, peer], row_rs.at[ls, x, at], peer, x
        )

    def meta_copy(peer, at):
        return remote(send_meta.at[peer], recv_meta.at[at], meta_ss.at[peer], meta_rs.at[at], peer, 0)

    table_copy = remote(
        desc.at[pl.ds(own * core_of(1), own)], table, table_sem.at[0], table_sem.at[1], me, 1
    )
    table_copy.start()
    far_first(lambda peer: meta_copy(peer, me).start())
    for ls in range(own):
        each_peer(lambda peer, x: row_copy(ls, peer, x, me).start(), far_first)
    local_meta = pltpu.make_async_copy(send_meta.at[me], recv_meta.at[me], local_sem.at[1])
    local_meta.start()
    local_rows = []
    for ls in range(own):
        local_rows.append(
            pltpu.make_async_copy(send.at[ls, 0, me], recv.at[ls, 0, me], local_sem.at[2 + ls])
        )
        local_rows[-1].start()

    step = 64
    entry = iota((n * hs, total), 0)
    column = iota((n * hs, total), 1)
    inside = column % slots
    unpack = [
        hot((entry == (column // slots) * hs + inside - g * hs) & (inside // hs == g)) for g in range(2)
    ]
    local_meta.wait()
    each_chip(lambda peer: meta_copy(peer, peer).wait_recv())
    arrived = recv_meta[...].reshape(n * hs, 128).astype(F32).T.astype(BF16)
    picks = []
    for ls in range(own):
        lists = sum(
            dot(arrived[(g * own + ls) * GROUP : (g * own + ls + 1) * GROUP], unpack[g]) for g in range(2)
        )
        picks.append(lists[k_count : k_count + 1])

        @pl.loop(0, cands // step)
        def _(i):
            ids = code(iota((step, total), 0) + i * step, cands).astype(F32)
            mask = ids == lists[0:1]
            for k in range(1, k_count):
                mask = mask | (ids == lists[k : k + 1])
            bias[ls, pl.ds(pl.multiple_of(i * step, step), step), :] = jnp.where(mask, 0.0, NEG)

    own_table.wait()
    table_copy.wait_recv()
    for ls in range(own):
        chosen = jnp.broadcast_to(picks[ls], (128, total)).T[:, 0:1]
        select = hot(chosen == code(iota((total, cands), 1), cands).astype(F32))
        taken[ls, 0] = dot(select, mine_table[ls])
        taken[ls, 1] = dot(select, table[ls])

    def back_copy(ls, peer, x, at):
        return remote(
            back.at[ls, x, peer], recv_back.at[ls, x, at],
            back_ss.at[ls, x, peer], back_rs.at[ls, x, at], peer, x,
        )

    def best_copy(peer, x, at):
        return remote(back_best.at[peer], recv_best.at[x, at], best_ss.at[x, peer], best_rs.at[x, at], peer, x)

    scale = 1.0 / math.sqrt(width)
    lane = iota((total, 128), 0)
    fold = None
    local_backs = []
    for ls in range(own):
        local_rows[ls].wait()
        each_peer(lambda peer, x: row_copy(ls, peer, x, peer).wait_recv())
        halves = [recv[ls, x].reshape(total, half) for x in range(2)]
        scores[...] = lax.dot_general(
            jnp.concatenate([mine_table[ls], table[ls]], axis=1), jnp.concatenate(halves, axis=1), NT,
            preferred_element_type=F32,
        )

        def chunk(i, carry):
            top, picked, claimed = carry
            at = pl.ds(pl.multiple_of(i * step, step), step)
            value = scores[at, :]
            masked = value + bias[ls, at, :]
            claim = jnp.max(masked, axis=1, keepdims=True)
            chosen = code(iota((step, total), 0) + i * step, cands).astype(F32) == picks[ls]

            def least(v):
                return jnp.max(v.reshape(step // 8, 8, total), axis=0)

            return (
                jnp.maximum(top, least(masked)),
                jnp.maximum(picked, least(jnp.where(chosen, value, NEG))),
                jnp.maximum(claimed, least(jnp.where(chosen, claim, NEG))),
            )

        start = jnp.full((8, total), NEG, F32)
        top, picked, claimed = [
            jnp.max(v, axis=0, keepdims=True)
            for v in lax.fori_loop(0, cands // step, chunk, (start, start, start))
        ]

        def quality(v):
            v = v * scale
            return 1.0 + jnp.maximum(v, 0.0) + jnp.log(1.0 + jnp.exp(-jnp.abs(v)))

        mine = quality(picked)
        share = mine / (mine + quality(claimed))
        share = jnp.broadcast_to(share, (128, total)).T
        for x in range(2):
            blend = (1.0 - share) * halves[x].astype(F32) + share * taken[ls, x]
            back[ls, x] = blend.astype(BF16).reshape(n, slots, half)

        top = jnp.where(top > NEG * 0.5, top * scale, 0.0)
        spread = jnp.where(
            iota((n, total), 0) == iota((n, total), 1) // slots, jnp.broadcast_to(top, (n, total)), 0.0
        ).astype(BF16)
        term = dot(spread, hot(iota((total, 128), 1) == ls * slots + lane % slots))
        fold = term if fold is None else fold + term
        if ls == own - 1:
            back_best[...] = fold.reshape(n, 1, 128)
            each_peer(lambda peer, x: best_copy(peer, x, me).start(), far_first)
        each_peer(lambda peer, x: back_copy(ls, peer, x, me).start(), far_first)
        local_backs.append(
            pltpu.make_async_copy(back.at[ls, 0, me], recv_back.at[ls, 0, me], local_sem.at[2 + own + ls])
        )
        local_backs[-1].start()
    local_best = pltpu.make_async_copy(back_best.at[me], recv_best.at[0, me], local_sem.at[2 + 2 * own])
    local_best.start()

    columns = [
        jnp.broadcast_to(target.astype(F32), (128, halos)).T[:, 0:1] for _, _, target, _ in route
    ]
    for ls in range(own):
        local_backs[ls].wait()
        each_peer(lambda peer, x: back_copy(ls, peer, x, peer).wait_recv())
        for x in range(2):
            s = own * core_of(x) + ls
            column = columns[x * own + ls]
            place = hot(iota((halos, total), 1).astype(F32) == column)
            rows = dot(place, recv_back[ls, x].reshape(total, half))
            phantom[s] = jnp.where(column < 0.0, halo[s].astype(F32), rows).astype(BF16)

    local_best.wait()
    each_peer(lambda peer, x: best_copy(peer, x, peer).wait_recv())
    tops = []
    for x in range(2):
        brought = recv_best[x].reshape(n, 128).astype(BF16)
        for ls in range(own):
            onehot, rank, _, live = route[x * own + ls]
            spread = lax.dot_general(brought, onehot, TN, preferred_element_type=F32)
            here = jnp.where(iota((128, halos), 0) == ls * slots + rank, spread, 0.0)
            tops.append(jnp.where(live, jnp.sum(here, axis=0, keepdims=True), 0.0))
    first, second = jnp.concatenate(tops[:own], axis=0), jnp.concatenate(tops[own:], axis=0)
    even = core == 0
    best[...] = jnp.concatenate(
        [jnp.where(even, first, second), jnp.where(even, second, first)], axis=0
    ).astype(BF16)

    table_copy.wait_send()
    each_chip(lambda peer: meta_copy(peer, me).wait_send())
    for ls in range(own):
        each_peer(lambda peer, x: row_copy(ls, peer, x, me).wait_send())
        each_peer(lambda peer, x: back_copy(ls, peer, x, me).wait_send())
    each_peer(lambda peer, x: best_copy(peer, x, me).wait_send())


def body(n, halo_rows, unmatched, owner_id, cand_index, lengths, choice_index, desc_rows):
    snaps, halos, half = halo_rows.shape
    cands = desc_rows.shape[1]
    own = snaps // 2
    slots = max(2 * halos // n, 16)
    total = n * slots
    dma = pltpu.SemaphoreType.DMA
    return pl.pallas_call(
        functools.partial(kernel, n, slots, 2 * half),
        out_shape=(
            jax.ShapeDtypeStruct((snaps, halos, half), BF16),
            jax.ShapeDtypeStruct((snaps, halos), BF16),
        ),
        in_specs=[pl.BlockSpec(memory_space=pltpu.VMEM)] * 6 + [pl.BlockSpec(memory_space=pl.ANY)],
        out_specs=(pl.BlockSpec(memory_space=pltpu.VMEM),) * 2,
        scratch_shapes=[
            pltpu.VMEM((own, 2, n, slots, half), BF16),
            pltpu.VMEM((own, 2, n, slots, half), BF16),
            pltpu.VMEM((n, slots // 2, 128), BF16),
            pltpu.VMEM((n, slots // 2, 128), BF16),
            pltpu.VMEM((own, cands, half), BF16),
            pltpu.VMEM((own, cands, half), BF16),
            pltpu.VMEM((cands, total), F32),
            pltpu.VMEM((own, cands, total), F32),
            pltpu.VMEM((own, 2, total, half), F32),
            pltpu.VMEM((own, 2, n, slots, half), BF16),
            pltpu.VMEM((own, 2, n, slots, half), BF16),
            pltpu.VMEM((n, 1, 128), F32),
            pltpu.VMEM((2, n, 1, 128), F32),
            dma((own, 2, n)), dma((own, 2, n)), dma((n,)), dma((n,)),
            dma((own, 2, n)), dma((own, 2, n)), dma((2, n)), dma((2, n)),
            dma((2,)), dma((3 + 2 * own,)),
        ],
        compiler_params=pltpu.CompilerParams(collective_id=0, has_side_effects=True),
    )(
        halo_rows,
        unmatched,
        jnp.swapaxes(owner_id, 1, 2),
        jnp.swapaxes(cand_index, 1, 2),
        lengths,
        choice_index,
        desc_rows,
    )


def solution(mesh):
    in_specs = (
        P(None, "space", "rep"),
        P(None, "space"),
        P(None, "space", None),
        P(None, "space", None),
        P(None, "space"),
        P(None, "space"),
        P(None, "space", "rep"),
    )
    out_specs = (P(None, "space", "rep"), P(None, "space"))
    return jax.shard_map(
        functools.partial(body, mesh.shape["space"]),
        mesh=mesh, in_specs=in_specs, out_specs=out_specs, check_vma=False,
    )
```

```python
import functools
import math

import jax
import jax.numpy as jnp
from jax import lax
from jax.experimental import pallas as pl
from jax.experimental.pallas import tpu as pltpu
from jax.sharding import PartitionSpec as P

MESH = pl.DeviceIdType.MESH
F32 = jnp.float32
BF16 = jnp.bfloat16
NEG = -1e30
GROUP = 32
NT = (((1,), (1,)), ((), ()))
TN = (((0,), (0,)), ((), ()))


def iota(shape, dim):
    return lax.broadcasted_iota(jnp.int32, shape, dim)


def dot(a, b):
    return jnp.dot(a, b, preferred_element_type=F32)


def hot(mask):
    return jnp.where(mask, 1.0, 0.0).astype(BF16)


def code(index, cands):
    return index - cands // 2 + jnp.where(index >= cands // 2, 1, 0)


def kernel(
    n, slots, width,
    halo_in, unmatched_in, owner_in, cand_in, lengths_in, choice_in, desc,
    phantom, best,
    halo, unmatched, owner, cand, lengths, choice,
    send, recv, send_meta, recv_meta, mine_table, table, scores, bias, taken,
    back, recv_back, back_best, recv_best,
    row_ss, row_rs, meta_ss, meta_rs, back_ss, back_rs, best_ss, best_rs, table_sem, local_sem, load_sem,
):
    me, core = lax.axis_index("space"), lax.axis_index("rep")
    snaps, halos, half = halo.shape
    k_count = cand.shape[1]
    cands = desc.shape[1]
    own = snaps // 2
    total = n * slots
    hs = slots // 2

    def core_of(x):
        return lax.rem(core + x, 2)

    def remote(src, dst, ss, rs, peer, x):
        return pltpu.make_async_remote_copy(
            src_ref=src, dst_ref=dst, send_sem=ss, recv_sem=rs,
            device_id=(peer, core_of(x)), device_id_type=MESH,
        )

    def each_chip(f):
        @pl.loop(1, n)
        def _(d):
            f(lax.rem(me + d, n))

    def each_peer(f):
        def both(peer):
            f(peer, 0)
            f(peer, 1)

        each_chip(both)
        f(me, 1)

    barrier = pltpu.get_barrier_semaphore()
    each_peer(
        lambda peer, x: pl.semaphore_signal(
            barrier, inc=1, device_id=(peer, core_of(x)), device_id_type=MESH
        ),
    )
    own_table = pltpu.make_async_copy(desc.at[pl.ds(own * core, own)], mine_table, local_sem.at[0])
    own_table.start()
    loads = [
        pltpu.make_async_copy(src, dst, load_sem.at[i])
        for i, (src, dst) in enumerate(
            [
                (owner_in, owner), (unmatched_in, unmatched), (cand_in, cand),
                (lengths_in, lengths), (choice_in, choice), (halo_in, halo),
            ]
        )
    ]
    for load in loads:
        load.start()
    for load in loads:
        load.wait()

    upper = hot(iota((halos, halos), 0) < iota((halos, halos), 1))
    route = []
    for x in range(2):
        for ls in range(own):
            s = own * core_of(x) + ls
            dest = owner[s]
            named = iota((n, halos), 0) == dest
            onehot = hot(named)
            rank = jnp.sum(jnp.where(named, dot(onehot, upper), 0.0), axis=0, keepdims=True)
            rank = rank.astype(jnp.int32)
            live = unmatched[pl.ds(s, 1), :] == 1
            target = jnp.where(live, dest * slots + rank, -1)
            route.append((onehot, rank, target, live))

    meta = None
    for ls in range(own):
        s = own * core + ls
        _, rank, _, live = route[ls]
        listed = code(cand[s], cands)
        k_ids = iota((k_count, halos), 0)
        pick = jnp.sum(jnp.where(k_ids == choice[pl.ds(s, 1), :], listed, 0), axis=0, keepdims=True)
        listed = jnp.where(k_ids < lengths[pl.ds(s, 1), :], listed, 0)
        block = jnp.concatenate(
            [listed, jnp.broadcast_to(pick, (GROUP - k_count, halos))], axis=0
        ).astype(F32)
        for g in range(2):
            lead = (g * own + ls) * GROUP
            parts = [jnp.zeros((lead, halos), F32)] if lead else []
            parts.append(block)
            if lead + GROUP < 128:
                parts.append(jnp.zeros((128 - lead - GROUP, halos), F32))
            here = live & (rank >= g * hs) & (rank < (g + 1) * hs)
            row = jnp.where(here, owner[s] * hs + rank - g * hs, -1)
            term = lax.dot_general(
                hot(iota((n * hs, halos), 0) == row),
                (jnp.concatenate(parts, axis=0) if len(parts) > 1 else block).astype(BF16),
                NT, preferred_element_type=F32,
            )
            meta = term if meta is None else meta + term
    send_meta[...] = meta.astype(BF16).reshape(n, hs, 128)

    for ls in range(own):
        for x in range(2):
            place = hot(iota((total, halos), 0) == route[x * own + ls][2])
            rows = dot(place, halo[own * core_of(x) + ls]).astype(BF16)
            send[ls, x] = rows.reshape(n, slots, half)

    pl.semaphore_wait(barrier, 2 * n - 1)

    def row_copy(ls, peer, x, at):
        return remote(
            send.at[ls, x, peer], recv.at[ls, x, at], row_ss.at[ls, x, peer], row_rs.at[ls, x, at], peer, x
        )

    def meta_copy(peer, at):
        return remote(send_meta.at[peer], recv_meta.at[at], meta_ss.at[peer], meta_rs.at[at], peer, 0)

    table_copy = remote(
        desc.at[pl.ds(own * core_of(1), own)], table, table_sem.at[0], table_sem.at[1], me, 1
    )
    table_copy.start()
    each_chip(lambda peer: meta_copy(peer, me).start())
    for ls in range(own):
        each_peer(lambda peer, x: row_copy(ls, peer, x, me).start())
    local_meta = pltpu.make_async_copy(send_meta.at[me], recv_meta.at[me], local_sem.at[1])
    local_meta.start()
    local_rows = []
    for ls in range(own):
        local_rows.append(
            pltpu.make_async_copy(send.at[ls, 0, me], recv.at[ls, 0, me], local_sem.at[2 + ls])
        )
        local_rows[-1].start()

    step = 64
    entry = iota((n * hs, total), 0)
    column = iota((n * hs, total), 1)
    inside = column % slots
    unpack = [
        hot((entry == (column // slots) * hs + inside - g * hs) & (inside // hs == g)) for g in range(2)
    ]
    local_meta.wait()
    each_chip(lambda peer: meta_copy(peer, peer).wait_recv())
    arrived = recv_meta[...].reshape(n * hs, 128).astype(F32).T.astype(BF16)
    picks = []
    for ls in range(own):
        lists = sum(
            dot(arrived[(g * own + ls) * GROUP : (g * own + ls + 1) * GROUP], unpack[g]) for g in range(2)
        )
        picks.append(lists[k_count : k_count + 1])

        @pl.loop(0, cands // step)
        def _(i):
            ids = code(iota((step, total), 0) + i * step, cands).astype(F32)
            mask = ids == lists[0:1]
            for k in range(1, k_count):
                mask = mask | (ids == lists[k : k + 1])
            bias[ls, pl.ds(pl.multiple_of(i * step, step), step), :] = jnp.where(mask, 0.0, NEG)

    own_table.wait()
    table_copy.wait_recv()
    for ls in range(own):
        chosen = jnp.broadcast_to(picks[ls], (128, total)).T[:, 0:1]
        select = hot(chosen == code(iota((total, cands), 1), cands).astype(F32))
        taken[ls, 0] = dot(select, mine_table[ls])
        taken[ls, 1] = dot(select, table[ls])

    def back_copy(ls, peer, x, at):
        return remote(
            back.at[ls, x, peer], recv_back.at[ls, x, at],
            back_ss.at[ls, x, peer], back_rs.at[ls, x, at], peer, x,
        )

    def best_copy(peer, x, at):
        return remote(back_best.at[peer], recv_best.at[x, at], best_ss.at[x, peer], best_rs.at[x, at], peer, x)

    scale = 1.0 / math.sqrt(width)
    lane = iota((total, 128), 0)
    fold = None
    local_backs = []
    for ls in range(own):
        local_rows[ls].wait()
        each_peer(lambda peer, x: row_copy(ls, peer, x, peer).wait_recv())
        halves = [recv[ls, x].reshape(total, half) for x in range(2)]
        scores[...] = lax.dot_general(
            jnp.concatenate([mine_table[ls], table[ls]], axis=1), jnp.concatenate(halves, axis=1), NT,
            preferred_element_type=F32,
        )

        def chunk(i, carry):
            top, picked, claimed = carry
            at = pl.ds(pl.multiple_of(i * step, step), step)
            value = scores[at, :]
            masked = value + bias[ls, at, :]
            claim = jnp.max(masked, axis=1, keepdims=True)
            chosen = code(iota((step, total), 0) + i * step, cands).astype(F32) == picks[ls]

            def least(v):
                return jnp.max(v.reshape(step // 8, 8, total), axis=0)

            return (
                jnp.maximum(top, least(masked)),
                jnp.maximum(picked, least(jnp.where(chosen, value, NEG))),
                jnp.maximum(claimed, least(jnp.where(chosen, claim, NEG))),
            )

        start = jnp.full((8, total), NEG, F32)
        top, picked, claimed = [
            jnp.max(v, axis=0, keepdims=True)
            for v in lax.fori_loop(0, cands // step, chunk, (start, start, start))
        ]

        def quality(v):
            v = v * scale
            return 1.0 + jnp.maximum(v, 0.0) + jnp.log(1.0 + jnp.exp(-jnp.abs(v)))

        mine = quality(picked)
        share = mine / (mine + quality(claimed))
        share = jnp.broadcast_to(share, (128, total)).T
        for x in range(2):
            blend = (1.0 - share) * halves[x].astype(F32) + share * taken[ls, x]
            back[ls, x] = blend.astype(BF16).reshape(n, slots, half)

        top = jnp.where(top > NEG * 0.5, top * scale, 0.0)
        spread = jnp.where(
            iota((n, total), 0) == iota((n, total), 1) // slots, jnp.broadcast_to(top, (n, total)), 0.0
        ).astype(BF16)
        term = dot(spread, hot(iota((total, 128), 1) == ls * slots + lane % slots))
        fold = term if fold is None else fold + term
        if ls == own - 1:
            back_best[...] = fold.reshape(n, 1, 128)
            each_peer(lambda peer, x: best_copy(peer, x, me).start())
        each_peer(lambda peer, x: back_copy(ls, peer, x, me).start())
        local_backs.append(
            pltpu.make_async_copy(back.at[ls, 0, me], recv_back.at[ls, 0, me], local_sem.at[2 + own + ls])
        )
        local_backs[-1].start()
    local_best = pltpu.make_async_copy(back_best.at[me], recv_best.at[0, me], local_sem.at[2 + 2 * own])
    local_best.start()

    columns = [
        jnp.broadcast_to(target.astype(F32), (128, halos)).T[:, 0:1] for _, _, target, _ in route
    ]
    for ls in range(own):
        local_backs[ls].wait()
        each_peer(lambda peer, x: back_copy(ls, peer, x, peer).wait_recv())
        for x in range(2):
            s = own * core_of(x) + ls
            column = columns[x * own + ls]
            place = hot(iota((halos, total), 1).astype(F32) == column)
            rows = dot(place, recv_back[ls, x].reshape(total, half))
            phantom[s] = jnp.where(column < 0.0, halo[s].astype(F32), rows).astype(BF16)

    local_best.wait()
    each_peer(lambda peer, x: best_copy(peer, x, peer).wait_recv())
    tops = []
    for x in range(2):
        brought = recv_best[x].reshape(n, 128).astype(BF16)
        for ls in range(own):
            onehot, rank, _, live = route[x * own + ls]
            spread = lax.dot_general(brought, onehot, TN, preferred_element_type=F32)
            here = jnp.where(iota((128, halos), 0) == ls * slots + rank, spread, 0.0)
            tops.append(jnp.where(live, jnp.sum(here, axis=0, keepdims=True), 0.0))
    first, second = jnp.concatenate(tops[:own], axis=0), jnp.concatenate(tops[own:], axis=0)
    even = core == 0
    best[...] = jnp.concatenate(
        [jnp.where(even, first, second), jnp.where(even, second, first)], axis=0
    ).astype(BF16)

    table_copy.wait_send()
    each_chip(lambda peer: meta_copy(peer, me).wait_send())
    for ls in range(own):
        each_peer(lambda peer, x: row_copy(ls, peer, x, me).wait_send())
        each_peer(lambda peer, x: back_copy(ls, peer, x, me).wait_send())
    each_peer(lambda peer, x: best_copy(peer, x, me).wait_send())


def hand_over(phantom_in, best_in, phantom, best):
    phantom[...] = phantom_in[...]
    best[...] = best_in[...]


def body(n, halo_rows, unmatched, owner_id, cand_index, lengths, choice_index, desc_rows):
    snaps, halos, half = halo_rows.shape
    cands = desc_rows.shape[1]
    own = snaps // 2
    slots = max(2 * halos // n, 16)
    total = n * slots
    dma = pltpu.SemaphoreType.DMA
    results = pl.pallas_call(
        functools.partial(kernel, n, slots, 2 * half),
        out_shape=(
            pltpu.VMEM((snaps, halos, half), BF16),
            pltpu.VMEM((snaps, halos), BF16),
        ),
        in_specs=[pl.BlockSpec(memory_space=pl.ANY)] * 7,
        out_specs=(pl.BlockSpec(memory_space=pltpu.VMEM),) * 2,
        scratch_shapes=[
            pltpu.VMEM(halo_rows.shape, BF16),
            pltpu.VMEM(unmatched.shape, jnp.int32),
            pltpu.VMEM((snaps, 1, halos), jnp.int32),
            pltpu.VMEM((snaps, cand_index.shape[2], halos), jnp.int32),
            pltpu.VMEM(lengths.shape, jnp.int32),
            pltpu.VMEM(choice_index.shape, jnp.int32),
            pltpu.VMEM((own, 2, n, slots, half), BF16),
            pltpu.VMEM((own, 2, n, slots, half), BF16),
            pltpu.VMEM((n, slots // 2, 128), BF16),
            pltpu.VMEM((n, slots // 2, 128), BF16),
            pltpu.VMEM((own, cands, half), BF16),
            pltpu.VMEM((own, cands, half), BF16),
            pltpu.VMEM((cands, total), F32),
            pltpu.VMEM((own, cands, total), F32),
            pltpu.VMEM((own, 2, total, half), F32),
            pltpu.VMEM((own, 2, n, slots, half), BF16),
            pltpu.VMEM((own, 2, n, slots, half), BF16),
            pltpu.VMEM((n, 1, 128), F32),
            pltpu.VMEM((2, n, 1, 128), F32),
            dma((own, 2, n)), dma((own, 2, n)), dma((n,)), dma((n,)),
            dma((own, 2, n)), dma((own, 2, n)), dma((2, n)), dma((2, n)),
            dma((2,)), dma((3 + 2 * own,)), dma((6,)),
        ],
        compiler_params=pltpu.CompilerParams(collective_id=0, has_side_effects=True),
    )(
        halo_rows,
        unmatched,
        jnp.swapaxes(owner_id, 1, 2),
        jnp.swapaxes(cand_index, 1, 2),
        lengths,
        choice_index,
        desc_rows,
    )
    shapes = tuple(jax.ShapeDtypeStruct(v.shape, v.dtype) for v in results)
    return pl.pallas_call(
        hand_over,
        out_shape=shapes,
        in_specs=[pl.BlockSpec(memory_space=pltpu.VMEM)] * 2,
        out_specs=(pl.BlockSpec(memory_space=pltpu.VMEM),) * 2,
    )(*[pltpu.with_memory_space_constraint(v, pltpu.VMEM) for v in results])


def solution(mesh):
    in_specs = (
        P(None, "space", "rep"),
        P(None, "space"),
        P(None, "space", None),
        P(None, "space", None),
        P(None, "space"),
        P(None, "space"),
        P(None, "space", "rep"),
    )
    out_specs = (P(None, "space", "rep"), P(None, "space"))
    return jax.shard_map(
        functools.partial(body, mesh.shape["space"]),
        mesh=mesh, in_specs=in_specs, out_specs=out_specs, check_vma=False,
    )
```
